32 devices in a mesh: lat: 8 (over y, x, core), rad: 4 (over z).
Axes of the slice: x: 2, y: 2, z: 4, core: 2. Of those that a mesh axis runs over, the one named last changes fastest.
Arguments:
- schur_off: bfloat16 [8, 4, 1536, 1536], P('lat', 'rad'), may hold values from -0.15625 to 0.15625
- schur_diag: float32 [8, 4, 1536], P('lat', 'rad'), may hold values from 1.5 to 4
- source: float32 [8, 4, 1536, 128], P('lat', 'rad'), may hold values from -6 to 6
- start: float32 [8, 4, 1536, 128], P('lat', 'rad'), may hold values from -6 to 6
- decay: float32 [8, 4, 256, 128], P('lat', 'rad'), may hold values from 0.2 to 1
- neighbour_face: int32 [8, 4], replicated, may hold values from 0 to 3
- orientation: int32 [8, 4], replicated, may hold values from 0 to 7
Outputs:
- traces: float32 [8, 4, 1536, 128], P('lat', 'rad')
The draws below stay inside these ranges and needn't reach their ends.
Inputs may be any that keep to these rules, and one draw needn't show every extreme that they name: `neighbour_face`: a face index of 0 to 3. `orientation`: a code of 0 to 7 whose bits select transpose, row reflection and column reflection.
All inputs are finite; a program needn't handle non-finite values.
Results may differ from the reference program's by a relative error of at most 0.001.
Values sent between devices are 32-bit elements; how exact they have to be, the bound alone decides.
A program may use at most 64 MiB of HBM per device.

```python
import math
import jax
import jax.numpy as jnp
import numpy as np
from jax import lax

FACE_SIDE = 16
FACE_NODES = 256
ORDER = 1536
COLS = 128
ITERS = 2
RADIAL_PASSES = 2
FAR = 2
N_LAT = 8
N_RAD = 4


def plant(array, stream_key, low, top_value):
    extent = array.shape
    place = [jax.random.randint(jax.random.fold_in(stream_key, axis), (), 0, extent[axis]) for axis in range(len(extent))]
    array = array.at[tuple(place)].set(low)
    longest = extent.index(max(extent))
    place[longest] = (place[longest] + 1) % extent[longest]
    return array.at[tuple(place)].set(top_value)


def steps_of(key, extent, cuts, smallest, largest):
    def one(dim, blocks):
        draws = jax.random.uniform(jax.random.fold_in(jax.random.fold_in(key, 6), dim), (blocks,), jnp.float32, smallest / len(cuts), largest / len(cuts))
        return jnp.repeat(jnp.exp(draws), extent[dim] // blocks).reshape((-1,) + (1,) * (len(extent) - dim - 1))

    gain = one(*cuts[0])
    for cut in cuts[1:]:
        gain = gain * one(*cut)
    return gain


def gaussian(own_key, extent, width, limit, shards=(), dtype=jnp.bfloat16):
    entries = jax.random.normal(own_key, extent, jnp.float32) * width
    if len(shards) > 0:
        entries = steps_of(own_key, extent, shards, -0.22, 0.18) * entries
    return jnp.clip(entries, min=-limit, max=limit).astype(dtype)


def setup_inputs(seed: int = 0) -> dict:
    seeds = jax.random.split(jax.random.key(seed), 8)
    return {
        "schur_off": gaussian(seeds[0], (N_LAT, N_RAD, ORDER, ORDER), ORDER ** -0.5, 0.15625, ((0, 8), (1, 4))),
        "schur_diag": jnp.clip(jnp.exp(math.log(4.0) - 0.98082925 * jax.random.uniform(seeds[1], (N_LAT, N_RAD, ORDER), jnp.float32) ** steps_of(seeds[1], (N_LAT, N_RAD, ORDER), ((0, 8), (1, 4)), -0.2, 0.2)), 1.5, 4.0),
        "source": gaussian(seeds[2], (N_LAT, N_RAD, ORDER, COLS), 1.0, 6.0, ((0, 8), (1, 4)), jnp.float32),
        "start": gaussian(seeds[3], (N_LAT, N_RAD, ORDER, COLS), 1.0, 6.0, ((0, 8), (1, 4)), jnp.float32),
        "decay": jnp.clip(0.2 + 0.8 * jax.random.uniform(seeds[4], (N_LAT, N_RAD, FACE_NODES, COLS), jnp.float32) ** steps_of(seeds[4], (N_LAT, N_RAD, FACE_NODES, COLS), ((0, 8), (1, 4)), -0.2, 0.2), 0.2, 1.0),
        "neighbour_face": plant(jax.random.randint(seeds[5], (N_LAT, 4), 0, 4), jax.random.fold_in(seeds[5], 1), 0, 3).astype(jnp.int32),
        "orientation": plant(jax.random.randint(seeds[6], (N_LAT, 4), 0, 8), jax.random.fold_in(seeds[6], 1), 0, 7).astype(jnp.int32),
    }


OMEGA = 0.3
COUPLE = 0.5


def orient_table(side):
    table = np.zeros((8, side * side), np.int32)
    for code in range(8):
        for i in range(side):
            for j in range(side):
                first, second = (j, i) if code & 1 else (i, j)
                if code & 2:
                    first = side - 1 - first
                if code & 4:
                    second = side - 1 - second
                table[code, i * side + j] = first * side + second
    return table


def apply_block(schur_off, schur_diag, trace):
    flat_w = schur_off.reshape(-1, ORDER, ORDER)
    flat_d = schur_diag.reshape(-1, ORDER)
    flat_u = trace.reshape(-1, ORDER, COLS)

    def single(items):
        weight, diag, value = items
        return jnp.dot(weight, value.astype(jnp.bfloat16), preferred_element_type=jnp.float32) + diag[:, None] * value

    return lax.map(single, (flat_w, flat_d, flat_u)).reshape(trace.shape)


def reference(schur_off, schur_diag, source, start, decay, neighbour_face, orientation):
    table = jnp.asarray(orient_table(FACE_SIDE))
    offsets = (-1, 1, -FAR, FAR)
    trace = start
    blank = jnp.zeros((N_LAT, N_RAD, FACE_NODES, COLS), jnp.float32)
    for outer in range(ITERS):
        applied = apply_block(schur_off, schur_diag, trace)
        faces = trace.reshape(N_LAT, N_RAD, 6, FACE_NODES, COLS)[:, :, :4]
        incoming = []
        for k in range(4):
            beside = jnp.roll(faces, -offsets[k], axis=0)
            pick = jnp.take_along_axis(beside, neighbour_face[:, k][:, None, None, None, None].astype(jnp.int32), axis=2)[:, :, 0]
            perm = table[orientation[:, k]]
            incoming.append(jnp.take_along_axis(pick, perm[:, None, :, None].astype(jnp.int32), axis=2))
        coupling = jnp.stack(incoming + [blank, blank], axis=2).reshape(trace.shape)
        trace = trace + OMEGA * (source - applied + COUPLE * coupling)
        for sweep in range(RADIAL_PASSES):
            res = source - apply_block(schur_off, schur_diag, trace)
            parts = res.reshape(N_LAT, N_RAD, 6, FACE_NODES, COLS)
            top = parts[:, :, 5]
            bottom = parts[:, :, 4]
            carry = jnp.zeros((N_LAT, FACE_NODES, COLS), jnp.float32)
            inflows = []
            for layer in range(N_RAD):
                inflows.append(carry)
                carry = decay[:, layer] * (carry + top[:, layer])
            inflow = jnp.stack(inflows, axis=1)
            above = jnp.concatenate([bottom[:, 1:], blank[:, :1]], axis=1)
            coupling = jnp.stack([blank, blank, blank, blank, inflow, above], axis=2).reshape(trace.shape)
            trace = trace + OMEGA * (res + COUPLE * coupling)
    return trace
```

```python
import functools
import math

import jax
import jax.numpy as jnp
from jax import lax
from jax.experimental import pallas as pl
from jax.experimental.pallas import tpu as pltpu
from jax.sharding import PartitionSpec as P

ITERS = 2
RADIAL_PASSES = 2
OMEGA = 0.3
COUPLE = 0.5
CHUNKS = 4
SEND_ORDER = (2, 3, 0, 1)
MESH = pl.DeviceIdType.MESH


def permuted(face, code, side):
    nodes = side * side
    n = lax.broadcasted_iota(jnp.int32, (nodes, 1), 0)
    i, j = n // side, n % side
    swap, rows, cols = code & 1, (code >> 1) & 1, (code >> 2) & 1
    a = i + swap * (j - i)
    b = j + swap * (i - j)
    a = a + rows * (side - 1 - 2 * a)
    b = b + cols * (side - 1 - 2 * b)
    at = lax.broadcasted_iota(jnp.int32, (nodes, nodes), 1)
    hot = jnp.where(at == a * side + b, 1.0, 0.0).astype(jnp.bfloat16)
    high = face.astype(jnp.bfloat16)
    rest = face - high.astype(jnp.float32)
    middle = rest.astype(jnp.bfloat16)
    low = (rest - middle.astype(jnp.float32)).astype(jnp.bfloat16)
    total = None
    for part in (low, middle, high):
        moved = jnp.dot(hot, part, preferred_element_type=jnp.float32)
        total = moved if total is None else total + moved
    return total


def kernel(
    lat_count, rad_count, nodes,
    face_at, code_at, diag_ref, w_hbm, source_hbm, start_hbm, decay_hbm,
    out_hbm,
    w, u, ub, rhs, factor, diag, res,
    lat_out, lat_in, dn_out, dn_in, h_out, h_in,
    load_sem, w_sem, out_sem,
    lat_send, lat_recv, dn_send, dn_recv, h_send, h_recv,
):
    side = math.isqrt(nodes)
    far = max(2, lat_count // 8)
    offsets = (-1, 1, -far, far)
    p = lax.axis_index("lat")
    r = lax.axis_index("rad")
    size = nodes // CHUNKS
    lanes = u.shape[1]
    upper, lower = slice(0, 4 * nodes), slice(4 * nodes, 6 * nodes)

    load_u = pltpu.make_async_copy(start_hbm.at[0, 0], u, load_sem.at[0])
    load_rhs = pltpu.make_async_copy(source_hbm.at[0, 0], rhs, load_sem.at[1])
    load_factor = pltpu.make_async_copy(decay_hbm.at[0, 0], factor, load_sem.at[2])
    load_w = [
        pltpu.make_async_copy(w_hbm.at[0, 0, part], w.at[part], w_sem.at[n])
        for n, part in enumerate((upper, lower))
    ]
    load_u.start()
    for copy in load_w:
        copy.start()
    load_rhs.start()
    load_factor.start()

    barrier = pltpu.get_barrier_semaphore()
    for offset in offsets:
        target = (p - offset + lat_count) % lat_count
        pl.semaphore_signal(barrier, inc=1, device_id={"lat": target}, device_id_type=MESH)

    below, above = (r - 1 + rad_count) % rad_count, (r + 1) % rad_count

    @pl.when(r > 0)
    def _():
        pl.semaphore_signal(barrier, inc=1, device_id={"rad": below}, device_id_type=MESH)

    @pl.when(r < rad_count - 1)
    def _():
        pl.semaphore_signal(barrier, inc=1, device_id={"rad": above}, device_id_type=MESH)

    inner = (r + rad_count - 1) // rad_count + (2 * rad_count - 2 - r) // rad_count
    pl.semaphore_wait(barrier, len(offsets) + inner)

    def lat_copy(outer, k):
        target = (p - offsets[k] + lat_count) % lat_count
        return pltpu.make_async_remote_copy(
            src_ref=lat_out.at[outer, k], dst_ref=lat_in.at[outer, k],
            send_sem=lat_send.at[outer, k], recv_sem=lat_recv.at[outer, k],
            device_id={"lat": target}, device_id_type=MESH,
        )

    def dn_copy(sweep):
        return pltpu.make_async_remote_copy(
            src_ref=dn_out.at[sweep], dst_ref=dn_in.at[sweep],
            send_sem=dn_send.at[sweep], recv_sem=dn_recv.at[sweep],
            device_id={"rad": below}, device_id_type=MESH,
        )

    def h_copy(sweep, c):
        rows = pl.ds(c * size, size)
        return pltpu.make_async_remote_copy(
            src_ref=h_out.at[sweep, rows], dst_ref=h_in.at[sweep, rows],
            send_sem=h_send.at[sweep, c], recv_sem=h_recv.at[sweep, c],
            device_id={"rad": above}, device_id_type=MESH,
        )

    def send_faces(outer):
        for k in SEND_ORDER:
            target = (p - offsets[k] + lat_count) % lat_count
            which = jnp.full((nodes, lanes), face_at[k, target], jnp.int32)
            face = u[slice(0, nodes), :]
            for f in range(1, 4):
                face = jnp.where(which == f, u[slice(f * nodes, (f + 1) * nodes), :], face)
            lat_out[outer, k] = permuted(face, code_at[k, target], side)
            lat_copy(outer, k).start()

    def residual(part):
        applied = jnp.dot(w[part, :], ub[...], preferred_element_type=jnp.float32)
        return rhs[part, :] - (applied + diag[part, :] * u[part, :])

    load_u.wait()
    send_faces(0)
    ub[...] = u[...].astype(jnp.bfloat16)
    for block in range(6 * nodes // lanes):
        own = slice(block * lanes, (block + 1) * lanes)
        diag[own, :] = jnp.broadcast_to(diag_ref[0, :, own], (lanes, lanes)).T
    load_rhs.wait()
    load_factor.wait()
    for copy in load_w:
        copy.wait()

    for outer in range(ITERS):
        for part in (upper, lower):
            res[part, :] = residual(part)
        u[lower, :] = u[lower, :] + OMEGA * res[lower, :]
        ub[lower, :] = u[lower, :].astype(jnp.bfloat16)
        for k in SEND_ORDER:
            own = slice(k * nodes, (k + 1) * nodes)
            lat_copy(outer, k).wait_recv()
            new = u[own, :] + OMEGA * (res[own, :] + COUPLE * lat_in[outer, k])
            u[own, :] = new
            ub[own, :] = new.astype(jnp.bfloat16)
        for turn in range(RADIAL_PASSES):
            sweep = outer * RADIAL_PASSES + turn
            bottom = slice(4 * nodes, 5 * nodes)
            top = slice(5 * nodes, 6 * nodes)
            res[lower, :] = residual(lower)

            @pl.when(r > 0)
            def _():
                dn_out[sweep] = res[bottom, :]
                dn_copy(sweep).start()

            @pl.when(r == 0)
            def _():
                h_out[sweep] = factor[...] * res[top, :]
                for c in range(CHUNKS):
                    h_copy(sweep, c).start()

            new = u[upper, :] + OMEGA * residual(upper)
            u[upper, :] = new
            ub[upper, :] = new.astype(jnp.bfloat16)
            if turn == RADIAL_PASSES - 1:
                if outer < ITERS - 1:
                    send_faces(outer + 1)
                else:
                    pltpu.make_async_copy(
                        u.at[upper], out_hbm.at[0, 0, upper], out_sem.at[0]
                    ).start()

            @pl.when(r > 0)
            def _():
                for c in range(CHUNKS):
                    rows = slice(c * size, (c + 1) * size)
                    from_bottom = slice(4 * nodes + c * size, 4 * nodes + (c + 1) * size)
                    from_top = slice(5 * nodes + c * size, 5 * nodes + (c + 1) * size)
                    h_copy(sweep, c).wait_recv()

                    @pl.when(r < rad_count - 1)
                    def _():
                        h_out[sweep, rows] = factor[rows, :] * (h_in[sweep, rows] + res[from_top, :])
                        h_copy(sweep, c).start()

                    u[from_bottom, :] = u[from_bottom, :] + OMEGA * (
                        res[from_bottom, :] + COUPLE * h_in[sweep, rows]
                    )

            @pl.when(r == 0)
            def _():
                u[bottom, :] = u[bottom, :] + OMEGA * res[bottom, :]

            @pl.when(r < rad_count - 1)
            def _():
                dn_copy(sweep).wait_recv()
                u[top, :] = u[top, :] + OMEGA * (res[top, :] + COUPLE * dn_in[sweep])

            @pl.when(r == rad_count - 1)
            def _():
                u[top, :] = u[top, :] + OMEGA * res[top, :]

            ub[lower, :] = u[lower, :].astype(jnp.bfloat16)

    out_copies = [
        pltpu.make_async_copy(u.at[part], out_hbm.at[0, 0, part], out_sem.at[n])
        for n, part in enumerate((upper, lower))
    ]
    out_copies[1].start()
    for outer in range(ITERS):
        for k in SEND_ORDER:
            lat_copy(outer, k).wait_send()

    @pl.when(r > 0)
    def _():
        for sweep in range(ITERS * RADIAL_PASSES):
            dn_copy(sweep).wait_send()

    @pl.when(r < rad_count - 1)
    def _():
        for sweep in range(ITERS * RADIAL_PASSES):
            for c in range(CHUNKS):
                h_copy(sweep, c).wait_send()

    for copy in out_copies:
        copy.wait()


def per_device(lat_count, rad_count, schur_off, schur_diag, source, start, decay, neighbour_face, orientation):
    order, columns = source.shape[2:]
    nodes = order // 6
    sweeps = ITERS * RADIAL_PASSES
    faces = lambda *lead: pltpu.VMEM((*lead, nodes, columns), jnp.float32)
    dma = lambda *shape: pltpu.SemaphoreType.DMA(shape)
    smem = pl.BlockSpec(memory_space=pltpu.SMEM)
    vmem = pl.BlockSpec(memory_space=pltpu.VMEM)
    hbm = pl.BlockSpec(memory_space=pl.ANY)
    return pl.pallas_call(
        functools.partial(kernel, lat_count, rad_count, nodes),
        out_shape=jax.ShapeDtypeStruct(source.shape, jnp.float32),
        in_specs=[smem, smem, vmem, hbm, hbm, hbm, hbm],
        out_specs=hbm,
        scratch_shapes=[
            pltpu.VMEM((order, order), jnp.bfloat16),
            pltpu.VMEM((order, columns), jnp.float32),
            pltpu.VMEM((order, columns), jnp.bfloat16),
            pltpu.VMEM((order, columns), jnp.float32),
            faces(),
            pltpu.VMEM((order, columns), jnp.float32),
            pltpu.VMEM((order, columns), jnp.float32),
            faces(ITERS, 4), faces(ITERS, 4), faces(sweeps), faces(sweeps), faces(sweeps), faces(sweeps),
            dma(3), dma(2), dma(2),
            dma(ITERS, 4), dma(ITERS, 4), dma(sweeps), dma(sweeps),
            dma(sweeps, CHUNKS), dma(sweeps, CHUNKS),
        ],
        compiler_params=pltpu.CompilerParams(
            collective_id=0, has_side_effects=True, vmem_limit_bytes=60 * 1024 * 1024
        ),
        name="shell",
    )(neighbour_face.T, orientation.T, schur_diag, schur_off, source, start, decay)


def solution(mesh):
    lat_count, rad_count = mesh.shape["lat"], mesh.shape["rad"]
    return jax.shard_map(
        functools.partial(per_device, lat_count, rad_count),
        mesh=mesh,
        in_specs=(
            P("lat", "rad", None, None),
            P("lat", "rad", None),
            P("lat", "rad", None, None),
            P("lat", "rad", None, None),
            P("lat", "rad", None, None),
            P(),
            P(),
        ),
        out_specs=P("lat", "rad", None, None),
        check_vma=False,
    )
```

```python
import functools
import math

import jax
import jax.numpy as jnp
from jax import lax
from jax.experimental import pallas as pl
from jax.experimental.pallas import tpu as pltpu
from jax.sharding import PartitionSpec as P

ITERS = 2
RADIAL_PASSES = 2
OMEGA = 0.3
COUPLE = 0.5
CHUNKS = 8
SEND_ORDER = (2, 3, 0, 1)
MESH = pl.DeviceIdType.MESH


def permuted(face, code, side):
    nodes = side * side
    n = lax.broadcasted_iota(jnp.int32, (nodes, 1), 0)
    i, j = n // side, n % side
    swap, rows, cols = code & 1, (code >> 1) & 1, (code >> 2) & 1
    a = i + swap * (j - i)
    b = j + swap * (i - j)
    a = a + rows * (side - 1 - 2 * a)
    b = b + cols * (side - 1 - 2 * b)
    at = lax.broadcasted_iota(jnp.int32, (nodes, nodes), 1)
    hot = jnp.where(at == a * side + b, 1.0, 0.0).astype(jnp.bfloat16)
    high = face.astype(jnp.bfloat16)
    rest = face - high.astype(jnp.float32)
    middle = rest.astype(jnp.bfloat16)
    low = (rest - middle.astype(jnp.float32)).astype(jnp.bfloat16)
    total = None
    for part in (low, middle, high):
        moved = jnp.dot(hot, part, preferred_element_type=jnp.float32)
        total = moved if total is None else total + moved
    return total


def kernel(
    lat_count, rad_count, nodes,
    face_at, code_at, diag_ref, w_hbm, source_hbm, start_hbm, decay_hbm,
    out_ref,
    w, ub, rhs, factor, diag, res, ready,
    lat_out, lat_in, dn_out, dn_in, h_out, h_in,
    load_sem, w_sem,
    lat_send, lat_recv, dn_send, dn_recv, h_send, h_recv,
):
    side = math.isqrt(nodes)
    far = max(2, lat_count // 8)
    offsets = (-1, 1, -far, far)
    p = lax.axis_index("lat")
    r = lax.axis_index("rad")
    size = nodes // CHUNKS
    u = out_ref.at[0, 0]
    lanes = u.shape[1]
    upper, lower = slice(0, 4 * nodes), slice(4 * nodes, 6 * nodes)

    load_u = pltpu.make_async_copy(start_hbm.at[0, 0], u, load_sem.at[0])
    load_rhs = pltpu.make_async_copy(source_hbm.at[0, 0], rhs, load_sem.at[1])
    load_factor = pltpu.make_async_copy(decay_hbm.at[0, 0], factor, load_sem.at[2])
    load_w = [
        pltpu.make_async_copy(w_hbm.at[0, 0, part], w.at[part], w_sem.at[n])
        for n, part in enumerate((upper, lower))
    ]
    load_u.start()
    for copy in load_w:
        copy.start()
    load_rhs.start()
    load_factor.start()

    barrier = pltpu.get_barrier_semaphore()
    for offset in offsets:
        target = (p - offset + lat_count) % lat_count
        pl.semaphore_signal(barrier, inc=1, device_id={"lat": target}, device_id_type=MESH)

    below, above = (r - 1 + rad_count) % rad_count, (r + 1) % rad_count

    @pl.when(r > 0)
    def _():
        pl.semaphore_signal(barrier, inc=1, device_id={"rad": below}, device_id_type=MESH)

    @pl.when(r < rad_count - 1)
    def _():
        pl.semaphore_signal(barrier, inc=1, device_id={"rad": above}, device_id_type=MESH)

    inner = (r + rad_count - 1) // rad_count + (2 * rad_count - 2 - r) // rad_count

    def lat_copy(outer, k):
        target = (p - offsets[k] + lat_count) % lat_count
        return pltpu.make_async_remote_copy(
            src_ref=lat_out.at[outer, k], dst_ref=lat_in.at[outer, k],
            send_sem=lat_send.at[outer, k], recv_sem=lat_recv.at[outer, k],
            device_id={"lat": target}, device_id_type=MESH,
        )

    def dn_copy(sweep):
        return pltpu.make_async_remote_copy(
            src_ref=dn_out.at[sweep], dst_ref=dn_in.at[sweep],
            send_sem=dn_send.at[sweep], recv_sem=dn_recv.at[sweep],
            device_id={"rad": below}, device_id_type=MESH,
        )

    def h_copy(sweep, c):
        rows = pl.ds(c * size, size)
        return pltpu.make_async_remote_copy(
            src_ref=h_out.at[sweep, rows], dst_ref=h_in.at[sweep, rows],
            send_sem=h_send.at[sweep, c], recv_sem=h_recv.at[sweep, c],
            device_id={"rad": above}, device_id_type=MESH,
        )

    def make_faces(outer, which_faces):
        for k in which_faces:
            target = (p - offsets[k] + lat_count) % lat_count
            which = jnp.full((nodes, lanes), face_at[k, target], jnp.int32)
            face = u[slice(0, nodes), :]
            for f in range(1, 4):
                face = jnp.where(which == f, u[slice(f * nodes, (f + 1) * nodes), :], face)
            lat_out[outer, k] = permuted(face, code_at[k, target], side)

    def start_faces(outer, which_faces):
        for k in which_faces:
            lat_copy(outer, k).start()

    def residual(part):
        applied = jnp.dot(w[part, :], ub[...], preferred_element_type=jnp.float32)
        return rhs[part, :] - (applied + diag[part, :] * u[part, :])

    load_u.wait()
    make_faces(0, SEND_ORDER[:2])
    pl.semaphore_wait(barrier, len(offsets) + inner)
    start_faces(0, SEND_ORDER[:2])
    for k in SEND_ORDER[2:]:
        make_faces(0, (k,))
        start_faces(0, (k,))
    ub[...] = u[...].astype(jnp.bfloat16)
    for block in range(6 * nodes // lanes):
        own = slice(block * lanes, (block + 1) * lanes)
        diag[own, :] = jnp.broadcast_to(diag_ref[0, :, own], (lanes, lanes)).T
    load_rhs.wait()
    load_factor.wait()
    for copy in load_w:
        copy.wait()

    for outer in range(ITERS):
        for part in (upper, lower):
            res[part, :] = residual(part)
        u[lower, :] = u[lower, :] + OMEGA * res[lower, :]
        ub[lower, :] = u[lower, :].astype(jnp.bfloat16)
        ready[...] = jnp.dot(w[lower, lower], ub[lower, :], preferred_element_type=jnp.float32)
        for k in SEND_ORDER:
            own = slice(k * nodes, (k + 1) * nodes)
            lat_copy(outer, k).wait_recv()
            new = u[own, :] + OMEGA * (res[own, :] + COUPLE * lat_in[outer, k])
            u[own, :] = new
            ub[own, :] = new.astype(jnp.bfloat16)
            if k != SEND_ORDER[-1]:
                ready[...] = ready[...] + jnp.dot(
                    w[lower, own], ub[own, :], preferred_element_type=jnp.float32
                )
        for turn in range(RADIAL_PASSES):
            sweep = outer * RADIAL_PASSES + turn
            bottom = slice(4 * nodes, 5 * nodes)
            top = slice(5 * nodes, 6 * nodes)
            last = slice(SEND_ORDER[-1] * nodes, (SEND_ORDER[-1] + 1) * nodes) if turn == 0 else lower
            applied = ready[...] + jnp.dot(
                w[lower, last], ub[last, :], preferred_element_type=jnp.float32
            )
            res[lower, :] = rhs[lower, :] - (applied + diag[lower, :] * u[lower, :])

            @pl.when(r > 0)
            def _():
                dn_out[sweep] = res[bottom, :]
                dn_copy(sweep).start()

            @pl.when(r == 0)
            def _():
                h_out[sweep] = factor[...] * res[top, :]
                for c in range(CHUNKS):
                    h_copy(sweep, c).start()

            new = u[upper, :] + OMEGA * residual(upper)
            u[upper, :] = new
            ub[upper, :] = new.astype(jnp.bfloat16)
            if turn == RADIAL_PASSES - 1:
                if outer < ITERS - 1:
                    for k in SEND_ORDER:
                        make_faces(outer + 1, (k,))
                        start_faces(outer + 1, (k,))
            else:
                ready[...] = jnp.dot(w[lower, upper], ub[upper, :], preferred_element_type=jnp.float32)

            @pl.when(r > 0)
            def _():
                for c in range(CHUNKS):
                    rows = slice(c * size, (c + 1) * size)
                    from_bottom = slice(4 * nodes + c * size, 4 * nodes + (c + 1) * size)
                    from_top = slice(5 * nodes + c * size, 5 * nodes + (c + 1) * size)
                    h_copy(sweep, c).wait_recv()

                    @pl.when(r < rad_count - 1)
                    def _():
                        h_out[sweep, rows] = factor[rows, :] * (h_in[sweep, rows] + res[from_top, :])
                        h_copy(sweep, c).start()

                    u[from_bottom, :] = u[from_bottom, :] + OMEGA * (
                        res[from_bottom, :] + COUPLE * h_in[sweep, rows]
                    )

            @pl.when(r == 0)
            def _():
                u[bottom, :] = u[bottom, :] + OMEGA * res[bottom, :]

            @pl.when(r < rad_count - 1)
            def _():
                dn_copy(sweep).wait_recv()
                u[top, :] = u[top, :] + OMEGA * (res[top, :] + COUPLE * dn_in[sweep])

            @pl.when(r == rad_count - 1)
            def _():
                u[top, :] = u[top, :] + OMEGA * res[top, :]

            ub[lower, :] = u[lower, :].astype(jnp.bfloat16)

    for outer in range(ITERS):
        for k in SEND_ORDER:
            lat_copy(outer, k).wait_send()

    @pl.when(r > 0)
    def _():
        for sweep in range(ITERS * RADIAL_PASSES):
            dn_copy(sweep).wait_send()

    @pl.when(r < rad_count - 1)
    def _():
        for sweep in range(ITERS * RADIAL_PASSES):
            for c in range(CHUNKS):
                h_copy(sweep, c).wait_send()


def per_device(lat_count, rad_count, schur_off, schur_diag, source, start, decay, neighbour_face, orientation):
    order, columns = source.shape[2:]
    nodes = order // 6
    sweeps = ITERS * RADIAL_PASSES
    faces = lambda *lead: pltpu.VMEM((*lead, nodes, columns), jnp.float32)
    dma = lambda *shape: pltpu.SemaphoreType.DMA(shape)
    smem = pl.BlockSpec(memory_space=pltpu.SMEM)
    vmem = pl.BlockSpec(memory_space=pltpu.VMEM)
    hbm = pl.BlockSpec(memory_space=pl.ANY)
    return pl.pallas_call(
        functools.partial(kernel, lat_count, rad_count, nodes),
        out_shape=jax.ShapeDtypeStruct(source.shape, jnp.float32),
        in_specs=[smem, smem, vmem, hbm, hbm, hbm, hbm],
        out_specs=vmem,
        scratch_shapes=[
            pltpu.VMEM((order, order), jnp.bfloat16),
            pltpu.VMEM((order, columns), jnp.bfloat16),
            pltpu.VMEM((order, columns), jnp.float32),
            faces(),
            pltpu.VMEM((order, columns), jnp.float32),
            pltpu.VMEM((order, columns), jnp.float32),
            pltpu.VMEM((2 * nodes, columns), jnp.float32),
            faces(ITERS, 4), faces(ITERS, 4), faces(sweeps), faces(sweeps), faces(sweeps), faces(sweeps),
            dma(3), dma(2),
            dma(ITERS, 4), dma(ITERS, 4), dma(sweeps), dma(sweeps),
            dma(sweeps, CHUNKS), dma(sweeps, CHUNKS),
        ],
        compiler_params=pltpu.CompilerParams(
            collective_id=0, has_side_effects=True, vmem_limit_bytes=63 * 1024 * 1024
        ),
        name="shell",
    )(neighbour_face.T, orientation.T, schur_diag, schur_off, source, start, decay)


def solution(mesh):
    lat_count, rad_count = mesh.shape["lat"], mesh.shape["rad"]
    return jax.shard_map(
        functools.partial(per_device, lat_count, rad_count),
        mesh=mesh,
        in_specs=(
            P("lat", "rad", None, None),
            P("lat", "rad", None),
            P("lat", "rad", None, None),
            P("lat", "rad", None, None),
            P("lat", "rad", None, None),
            P(),
            P(),
        ),
        out_specs=P("lat", "rad", None, None),
        check_vma=False,
    )
```
